32 devices in a mesh: dp: 8 (over y, x, core), mp: 4 (over z).
Axes of the slice: x: 2, y: 2, z: 4, core: 2. Of those that a mesh axis runs over, the one named last changes fastest.
Arguments:
- candidates: bfloat16 [64, 256, 768], P('dp', 'mp'), may hold values from -6 to 6
- owner_row: int32 [64], replicated, may hold values from 0 to 63, as said below
- selected: int32 [16], replicated, may hold values from 0 to 63, as said below
- dest_slot: int32 [16], replicated, may hold values from 0 to 15, as said below
- patch_weight: bfloat16 [768, 768], P(None, 'mp'), may hold values from -0.21875 to 0.21875
- positions: bfloat16 [256, 768], P(None, 'mp'), may hold values from -3 to 3
- qkv_weight: bfloat16 [768, 3, 768], P(None, None, 'mp'), may hold values from -1 to 1
- out_weight: bfloat16 [768, 768], P('mp'), may hold values from -0.21875 to 0.21875
- attn_gain: bfloat16 [768], replicated, may hold values from 0.099609375 to 1.8984375
- mlp_gain: bfloat16 [768], replicated, may hold values from 0.099609375 to 1.8984375
- up_weight: bfloat16 [768, 3072], P(None, 'mp'), may hold values from -0.21875 to 0.21875
- down_weight: bfloat16 [3072, 768], P('mp'), may hold values from -0.109375 to 0.109375
Outputs:
- layer_out: bfloat16 [16, 256, 768], P('dp', 'mp')
The draws below stay inside these ranges and needn't reach their ends.
Inputs may be any that keep to these rules, and one draw needn't show every extreme that they name: `owner_row`: a permutation; storage row r sits on index r // 8 of dp. `selected`: distinct candidates; no index of dp stores more than 4 of them, and some index stores exactly 4. `dest_slot`: a permutation; the 2 slots s with equal s // 2 get candidates stored on different indices of dp.
All inputs are finite; a program needn't handle non-finite values.
Results may differ from the reference program's by a relative error of at most 0.012.
Values may be sent and summed in bfloat16 or wider, within the bound.
A program may use at most 128 MiB of HBM per device.

```python
import math
import jax
import jax.numpy as jnp
from jax import lax

D = 768
HEADS = 12
FF = 3072
PIX = 768
PATCHES = 256
CAND_DEV = 8
SEL_DEV = 2
MOST = 4
HEAD_DIM = 64
CANDS = 64
SEL = 16
N_MP = 4


def routing_plan(key):
    subkeys = jax.random.split(jax.random.fold_in(key, 41), 5)
    learners = SEL // SEL_DEV
    owner_row = jax.random.permutation(subkeys[0], CANDS).astype(jnp.int32)
    placing = jax.random.permutation(subkeys[1], learners).astype(jnp.int32)
    position = jnp.argsort(placing).astype(jnp.int32)
    group_index = position // MOST
    within = position % MOST
    counts = jnp.where(group_index % 2 == 0, jnp.where(within < SEL_DEV, MOST, 0), SEL_DEV).astype(jnp.int32)
    run_end = jnp.cumsum(counts).astype(jnp.int32)
    starts = run_end - counts
    series = jnp.arange(SEL, dtype=jnp.int32)
    owners = jnp.sum((run_end[None, :] <= series[:, None]).astype(jnp.int32), axis=1).astype(jnp.int32)
    local_rank = series - starts[owners]
    shuffles = jax.vmap(lambda sub: jax.random.permutation(sub, CAND_DEV))(jax.random.split(subkeys[2], learners)).astype(jnp.int32)
    storage = owners * CAND_DEV + shuffles[owners, local_rank]
    inverse = jnp.argsort(owner_row).astype(jnp.int32)
    chosen = inverse[storage]
    learner_order = jax.random.permutation(subkeys[3], learners).astype(jnp.int32)
    slot_index = learner_order[series % learners] * SEL_DEV + series // learners
    mixing = jax.random.permutation(subkeys[4], SEL).astype(jnp.int32)
    return (owner_row, chosen[mixing].astype(jnp.int32), slot_index[mixing].astype(jnp.int32))


def draw_owner_row(key, part):
    return routing_plan(key)[0]


def draw_selected(key, part):
    return routing_plan(key)[1]


def draw_dest_slot(key, part):
    return routing_plan(key)[2]


def draw_qkv_weight(key, part):
    base = jax.random.normal(key, (D, 3, D), jnp.float32) / math.sqrt(D)
    return jnp.clip(base, -1.0, 1.0).astype(jnp.bfloat16)


def level_of(stream_key, dims, shards, least, high):
    loudness = 1.0
    for axis_at, shards_of in shards:
        steps = jax.random.uniform(jax.random.fold_in(jax.random.fold_in(stream_key, 6), axis_at), (shards_of,), jnp.float32, least / len(shards), high / len(shards))
        loudness = loudness * jnp.repeat(jnp.exp(steps), dims[axis_at] // shards_of).reshape((-1,) + (1,) * (len(dims) - 1 - axis_at))
    return loudness


def normal_values(own_key, shape, scale, most, cuts=(), held_as=jnp.bfloat16):
    result = jax.random.normal(own_key, shape, jnp.float32) * scale
    if len(cuts) > 0:
        result = level_of(own_key, shape, cuts, -0.22, 0.18) * result
    return jnp.clip(result, min=-most, max=most).astype(held_as)


def setup_inputs(seed: int = 0) -> dict:
    key_of = jax.random.split(jax.random.key(seed), 13)
    return {
        "candidates": normal_values(key_of[0], (CANDS, PATCHES, PIX), 1.0, 6.0, ((0, 8), (1, 4))),
        "owner_row": draw_owner_row(jax.random.fold_in(key_of[12], 71), 0),
        "selected": draw_selected(jax.random.fold_in(key_of[12], 71), 0),
        "dest_slot": draw_dest_slot(jax.random.fold_in(key_of[12], 71), 0),
        "patch_weight": normal_values(key_of[4], (PIX, D), PIX ** -0.5, 0.21875, ((1, 4),)),
        "positions": normal_values(key_of[5], (PATCHES, D), 0.5, 3.0, ((1, 4),)),
        "qkv_weight": draw_qkv_weight(jax.random.fold_in(key_of[12], 71), 0),
        "out_weight": normal_values(key_of[7], (D, D), D ** -0.5, 0.21875, ((0, 4),)),
        "attn_gain": jnp.clip(1.0 + 0.18 * jax.random.normal(key_of[8], (D,), jnp.float32), 0.099609375, 1.8984375).astype(jnp.bfloat16),
        "mlp_gain": jnp.clip(1.0 + 0.18 * jax.random.normal(key_of[9], (D,), jnp.float32), 0.099609375, 1.8984375).astype(jnp.bfloat16),
        "up_weight": normal_values(key_of[10], (D, FF), D ** -0.5, 0.21875, ((1, 4),)),
        "down_weight": normal_values(key_of[11], (FF, D), FF ** -0.5, 0.109375, ((0, 4),)),
    }


def norm_rows(values, gain):
    average = lax.optimization_barrier(jnp.mean(values, axis=-1, keepdims=True))
    centred = values - average
    variance = lax.optimization_barrier(jnp.mean(centred * centred, axis=-1, keepdims=True))
    return centred * lax.rsqrt(variance + 1e-06) * gain.astype(jnp.float32)

def group_sum(left, right, groups):
    count = left.shape[0]
    left_groups = left.reshape(count, groups, left.shape[1] // groups).astype(jnp.float32)
    right_groups = right.reshape(groups, right.shape[0] // groups, right.shape[1]).astype(jnp.float32)
    partials = jnp.einsum('tgk,gkd->tgd', left_groups, right_groups)
    rounded = lax.optimization_barrier(partials.astype(jnp.bfloat16))
    return lax.optimization_barrier(jnp.sum(rounded.astype(jnp.float32), axis=1))

def layer_one(pixels, patch_weight, positions, qkv_weight, out_weight, attn_gain, mlp_gain, up_weight, down_weight):
    embedded = (jnp.dot(pixels, patch_weight, preferred_element_type=jnp.float32) + positions.astype(jnp.float32)).astype(jnp.bfloat16)
    activations = embedded.astype(jnp.float32)
    normed = norm_rows(activations, attn_gain).astype(jnp.bfloat16)
    projected = jnp.einsum('td,dce->tce', normed.astype(jnp.float32), qkv_weight.astype(jnp.float32)).astype(jnp.bfloat16)
    head_split = projected.reshape(PATCHES, 3, HEADS, HEAD_DIM).astype(jnp.float32)
    queries = head_split[:, 0]
    attn_keys = head_split[:, 1]
    attn_values = head_split[:, 2]
    scores = jnp.einsum('qhd,khd->hqk', queries, attn_keys) * HEAD_DIM ** (-0.5)
    attn_probs = jax.nn.softmax(scores, axis=-1).astype(jnp.bfloat16)
    context = jnp.einsum('hqk,khd->qhd', attn_probs.astype(jnp.float32), attn_values).astype(jnp.bfloat16)
    context = context.reshape(PATCHES, D)
    attended = group_sum(context, out_weight, N_MP)
    after_attn = activations + attended
    normed2 = norm_rows(after_attn, mlp_gain).astype(jnp.bfloat16)
    hidden = jax.nn.gelu(jnp.dot(normed2, up_weight, preferred_element_type=jnp.float32), approximate=False).astype(jnp.bfloat16)
    feed = group_sum(hidden, down_weight, N_MP)
    return (after_attn + feed).astype(jnp.bfloat16)

def reference(candidates, owner_row, selected, dest_slot, patch_weight, positions, qkv_weight, out_weight, attn_gain, mlp_gain, up_weight, down_weight):
    chosen_rows = jnp.take(owner_row, selected).astype(jnp.int32)
    slot_rows = jnp.zeros((SEL,), jnp.int32).at[dest_slot].set(chosen_rows)
    batch = jnp.take(candidates, slot_rows, axis=0)

    def one_example(pixels):
        return layer_one(pixels, patch_weight, positions, qkv_weight, out_weight, attn_gain, mlp_gain, up_weight, down_weight)
    return lax.map(one_example, batch)
```

```python
import functools

import jax
import jax.numpy as jnp
from jax import lax
from jax.experimental import pallas as pl
from jax.experimental.pallas import tpu as pltpu
from jax.sharding import PartitionSpec as P

HEAD_DIM = 64
MESH = pl.DeviceIdType.MESH


def norm_rows(values, gain):
    average = jnp.mean(values, axis=-1, keepdims=True)
    centred = values - average
    variance = jnp.mean(centred * centred, axis=-1, keepdims=True)
    return centred * lax.rsqrt(variance + 1e-06) * gain


def dot(a, b):
    return jnp.dot(a, b, preferred_element_type=jnp.float32)


def kernel(
    n_dp, n_mp, stored, per,
    owner_row, selected, dest_slot,
    cand, pw, pos, qkv, out_w, gain1, gain2, up, down,
    out,
    send, recv, wbuf, pbuf, xbuf, act, after, ctx, ag1, part1, ra1, rm1, rb1, ag2, part2, ra2, rm2, rb2,
    route_s, route_r, w_s, w_r, d_s, d_r, p_s, p_r, ag_s, ag_r, rs_s, rs_r, loc,
):
    dp = lax.axis_index("dp")
    mp = lax.axis_index("mp")
    quarter, width = cand.shape[1], cand.shape[2]
    feats = pw.shape[1]
    half = pw.shape[0] // 2
    side = mp + 1 - 2 * lax.rem(mp, 2)
    across = lax.rem(mp + n_mp // 2, n_mp)
    corner = n_mp - 1 - mp
    twin = dp + 1 - 2 * lax.rem(dp, 2)

    barrier = pltpu.get_barrier_semaphore()
    for other in (side, across, corner):
        pl.semaphore_signal(barrier, inc=1, device_id=(dp, other), device_id_type=MESH)

    @pl.loop(1, n_dp)
    def _(k):
        pl.semaphore_signal(barrier, inc=1, device_id=(lax.rem(dp + k, n_dp), mp), device_id_type=MESH)

    own_w = pltpu.make_async_copy(pw, wbuf.at[mp], loc.at[0])
    own_p = pltpu.make_async_copy(pos.at[pl.ds(mp * quarter, quarter)], pbuf.at[mp], loc.at[1])
    own_w.start()
    own_p.start()

    count = selected.shape[0]

    def row_of(i):
        return owner_row[selected[i]]

    def pick(learner):
        def body(i, found):
            row = row_of(i)
            hit = (lax.div(dest_slot[i], per) == learner) & (lax.div(row, stored) == dp)
            return jnp.where(hit, lax.rem(row, stored), found)
        return lax.fori_loop(0, count, body, jnp.int32(0), unroll=count <= 16)

    def sender(slot):
        def body(i, found):
            return jnp.where(dest_slot[i] == slot, lax.div(row_of(i), stored), found)
        return lax.fori_loop(0, count, body, jnp.int32(0), unroll=count <= 16)

    recv[dp] = cand[pick(dp)]

    @pl.loop(1, n_dp)
    def _(k):
        learner = lax.rem(dp + n_dp - k, n_dp)
        send[learner] = cand[pick(learner)]

    pl.semaphore_wait(barrier, 3 + n_dp - 1)

    def remote(src, dst, ss, rs, where):
        return pltpu.make_async_remote_copy(
            src_ref=src, dst_ref=dst, send_sem=ss, recv_sem=rs, device_id=where, device_id_type=MESH
        )

    mine = pl.ds(pl.multiple_of(lax.rem(dp, 2) * half, half), half)
    w_side = remote(pw.at[mine], wbuf.at[mp, mine], w_s.at[0], w_r.at[0], (dp, side))
    w_across = remote(pw.at[mine], wbuf.at[mp, mine], w_s.at[1], w_r.at[1], (dp, across))
    w_across.start()
    w_side.start()
    p_copies = []
    for j, other in enumerate((side, across, corner)):
        c = remote(pos.at[pl.ds(other * quarter, quarter)], pbuf.at[mp], p_s.at[j], p_r.at[j], (dp, other))
        c.start()
        p_copies.append(c)

    @pl.loop(1, n_dp)
    def _(k):
        learner = lax.rem(dp + n_dp - k, n_dp)
        remote(send.at[learner], recv.at[dp], route_s.at[learner], route_r.at[dp], (learner, mp)).start()

    w_across.wait_recv()
    w_fwd = remote(wbuf.at[across, mine], wbuf.at[across, mine], w_s.at[2], w_r.at[2], (dp, side))
    w_fwd.start()
    d_copies = []

    def to_twin(j, block):
        c = remote(wbuf.at[block, mine], wbuf.at[block, mine], d_s.at[j], d_r.at[j], (twin, mp))
        c.start()
        d_copies.append(c)

    to_twin(0, across)
    w_side.wait_recv()
    to_twin(1, side)
    w_fwd.wait_recv()
    to_twin(2, corner)
    for c in p_copies:
        c.wait()

    @pl.loop(1, n_dp)
    def _(k):
        peer = lax.rem(dp + k, n_dp)
        remote(send.at[peer], recv.at[peer], route_s.at[peer], route_r.at[peer], (peer, mp)).wait()

    own_w.wait()
    own_p.wait()
    for e in range(per):
        xbuf[e * quarter:(e + 1) * quarter] = recv[sender(dp * per + e)]
    for c in d_copies:
        c.wait()
    for c in (w_side, w_across, w_fwd):
        c.wait_send()

    for g in range(n_mp):
        prod = dot(xbuf[...], wbuf[g])
        place = jnp.concatenate([pbuf[g].astype(jnp.float32)] * per, axis=0)
        act[:, g * feats:(g + 1) * feats] = (prod + place).astype(jnp.bfloat16).astype(jnp.float32)

    def gather_start(buf, base, e):
        cs = []
        for j, other in enumerate((across, side)):
            c = remote(buf.at[e, mp], buf.at[e, mp], ag_s.at[base + j], ag_r.at[base + j], (dp, other))
            c.start()
            cs.append(c)
        return cs

    def gather_forward(buf, base, e, cs):
        cs[0].wait_recv()
        c = remote(buf.at[e, across], buf.at[e, across], ag_s.at[base + 2], ag_r.at[base + 2], (dp, side))
        c.start()
        cs.append(c)

    def gather_end(cs):
        cs[1].wait_recv()
        cs[2].wait_recv()
        for c in cs:
            c.wait_send()

    def sum_start(part, ra, base, e):
        cs = []
        for j, block in enumerate((corner, side)):
            c = remote(part.at[e, block], ra.at[e, j], rs_s.at[base + j], rs_r.at[base + j], (dp, side))
            c.start()
            cs.append(c)
        return cs

    def sum_merge(part, ra, rm, rb, base, e, cs):
        cs[0].wait_recv()
        rm[e] = (part[e, across].astype(jnp.float32) + ra[e, 0].astype(jnp.float32)).astype(jnp.bfloat16)
        c = remote(rm.at[e], rb.at[e], rs_s.at[base + 2], rs_r.at[base + 2], (dp, across))
        c.start()
        cs.append(c)

    def sum_end(part, ra, rb, e, cs):
        cs[1].wait_recv()
        cs[2].wait_recv()
        for c in cs:
            c.wait_send()
        return part[e, mp].astype(jnp.float32) + ra[e, 1].astype(jnp.float32) + rb[e].astype(jnp.float32)

    def rows(e):
        return pl.ds(e * quarter, quarter)

    g1 = gain1[...].astype(jnp.float32)
    g2 = gain2[...].astype(jnp.float32)
    every = range(per)
    gathers = []
    for e in every:
        ag1[e, mp] = norm_rows(act[rows(e)], g1).astype(jnp.bfloat16)
        gathers.append(gather_start(ag1, 3 * e, e))
    for e in every:
        gather_forward(ag1, 3 * e, e, gathers[e])

    tokens = n_mp * quarter
    sums = []
    for e in every:
        gather_end(gathers[e])
        normed = ag1[e].reshape(tokens, width)
        q = (dot(normed, qkv[0]) .astype(jnp.bfloat16) * HEAD_DIM ** (-0.5)).astype(jnp.bfloat16)
        k = dot(normed, qkv[1]).astype(jnp.bfloat16)
        v = dot(normed, qkv[2]).astype(jnp.bfloat16)
        for h in range(feats // HEAD_DIM):
            cut = slice(h * HEAD_DIM, (h + 1) * HEAD_DIM)
            s = lax.dot_general(q[:, cut], k[:, cut], (((1,), (1,)), ((), ())), preferred_element_type=jnp.float32)
            p = jnp.exp(s - jnp.max(s, axis=-1, keepdims=True))
            total = jnp.sum(p, axis=-1, keepdims=True)
            ctx[:, cut] = (dot(p.astype(jnp.bfloat16), v[:, cut]) / total).astype(jnp.bfloat16)
        part1[e] = dot(ctx[...], out_w[...]).astype(jnp.bfloat16).reshape(n_mp, quarter, width)
        sums.append(sum_start(part1, ra1, 3 * e, e))
    for e in every:
        sum_merge(part1, ra1, rm1, rb1, 3 * e, e, sums[e])
    gathers = []
    for e in every:
        value = act[rows(e)] + sum_end(part1, ra1, rb1, e, sums[e])
        after[rows(e)] = value
        ag2[e, mp] = norm_rows(value, g2).astype(jnp.bfloat16)
        gathers.append(gather_start(ag2, 3 * (per + e), e))
    for e in every:
        gather_forward(ag2, 3 * (per + e), e, gathers[e])
    sums = []
    for e in every:
        gather_end(gathers[e])
        x = dot(ag2[e].reshape(tokens, width), up[...])
        hidden = (0.5 * x * (1.0 + lax.erf(x * 0.7071067811865476))).astype(jnp.bfloat16)
        part2[e] = dot(hidden, down[...]).astype(jnp.bfloat16).reshape(n_mp, quarter, width)
        sums.append(sum_start(part2, ra2, 3 * (per + e), e))
    for e in every:
        sum_merge(part2, ra2, rm2, rb2, 3 * (per + e), e, sums[e])
    for e in every:
        out[e] = (after[rows(e)] + sum_end(part2, ra2, rb2, e, sums[e])).astype(jnp.bfloat16)


def solution(mesh):
    n_dp, n_mp = mesh.shape["dp"], mesh.shape["mp"]

    def local(
        candidates, owner_row, selected, dest_slot, patch_weight, positions,
        qkv_weight, out_weight, attn_gain, mlp_gain, up_weight, down_weight,
    ):
        stored, quarter, width = candidates.shape
        per = selected.shape[0] // n_dp
        feats = patch_weight.shape[1]
        qkv = jnp.transpose(qkv_weight, (1, 0, 2))
        vm = pl.BlockSpec(memory_space=pltpu.VMEM)
        sm = pl.BlockSpec(memory_space=pltpu.SMEM)
        bf, f32 = jnp.bfloat16, jnp.float32
        blocks = pltpu.VMEM((per, n_mp, quarter, width), bf)
        pair = pltpu.VMEM((per, 2, quarter, width), bf)
        one = pltpu.VMEM((per, quarter, width), bf)
        dma = pltpu.SemaphoreType.DMA
        return pl.pallas_call(
            functools.partial(kernel, n_dp, n_mp, stored, per),
            out_shape=jax.ShapeDtypeStruct((per, quarter, width), bf),
            in_specs=[sm] * 3 + [vm] * 9,
            out_specs=vm,
            scratch_shapes=[
                pltpu.VMEM((n_dp, quarter, width), bf),
                pltpu.VMEM((n_dp, quarter, width), bf),
                pltpu.VMEM((n_mp, width, feats), bf),
                pltpu.VMEM((n_mp, quarter, feats), bf),
                pltpu.VMEM((per * quarter, width), bf),
                pltpu.VMEM((per * quarter, n_mp * feats), f32),
                pltpu.VMEM((per * quarter, n_mp * feats), f32),
                pltpu.VMEM((n_mp * quarter, feats), bf),
                blocks, blocks, pair, one, one,
                blocks, blocks, pair, one, one,
                dma((n_dp,)), dma((n_dp,)),
                dma((3,)), dma((3,)), dma((3,)), dma((3,)), dma((3,)), dma((3,)),
                dma((6 * per,)), dma((6 * per,)), dma((6 * per,)), dma((6 * per,)),
                dma((2,)),
            ],
            compiler_params=pltpu.CompilerParams(
                collective_id=0, has_side_effects=True, vmem_limit_bytes=60000 * 1024
            ),
        )(
            owner_row, selected, dest_slot, candidates, patch_weight, positions, qkv, out_weight,
            attn_gain.reshape(1, -1), mlp_gain.reshape(1, -1), up_weight, down_weight,
        )

    return jax.shard_map(
        local,
        mesh=mesh,
        in_specs=(
            P("dp", "mp", None), P(), P(), P(), P(None, "mp"), P(None, "mp"), P(None, None, "mp"),
            P("mp", None), P(), P(), P(None, "mp"), P("mp", None),
        ),
        out_specs=P("dp", "mp", None),
        check_vma=False,
    )
```

```python
import functools

import jax
import jax.numpy as jnp
from jax import lax
from jax.experimental import pallas as pl
from jax.experimental.pallas import tpu as pltpu
from jax.sharding import PartitionSpec as P

HEAD_DIM = 64
MESH = pl.DeviceIdType.MESH


def norm_rows(values, gain):
    average = jnp.mean(values, axis=-1, keepdims=True)
    centred = values - average
    variance = jnp.mean(centred * centred, axis=-1, keepdims=True)
    return centred * lax.rsqrt(variance + 1e-06) * gain


def dot(a, b):
    return jnp.dot(a, b, preferred_element_type=jnp.float32)


def dot_t(a, b):
    return lax.dot_general(a, b, (((1,), (1,)), ((), ())), preferred_element_type=jnp.float32)


def kernel(
    n_dp, n_mp, stored, per,
    owner_row, selected, dest_slot,
    cand, pw, pos_t, gain1, gain2, qkv_h, out_h, up_h, down_h,
    out,
    qkv, out_w, up, down, pos,
    send, recv, wbuf, pbuf, xbuf, act, after, ctx, ag1, part1, ra1, rm1, rb1, ag2, part2, ra2, rm2, rb2,
    route_s, route_r, w_s, w_r, d_s, d_r, p_s, p_r, ag_s, ag_r, rs_s, rs_r, loc,
):
    dp = lax.axis_index("dp")
    mp = lax.axis_index("mp")
    quarter, width = cand.shape[1], cand.shape[2]
    feats = pw.shape[0]
    half = feats // 2
    side = mp + 1 - 2 * lax.rem(mp, 2)
    across = lax.rem(mp + n_mp // 2, n_mp)
    corner = n_mp - 1 - mp
    twin = dp + 1 - 2 * lax.rem(dp, 2)

    barrier = pltpu.get_barrier_semaphore()
    for other in (side, across, corner):
        pl.semaphore_signal(barrier, inc=1, device_id=(dp, other), device_id_type=MESH)

    @pl.loop(1, n_dp)
    def _(k):
        pl.semaphore_signal(barrier, inc=1, device_id=(lax.rem(dp + k, n_dp), mp), device_id_type=MESH)

    own_w = pltpu.make_async_copy(pw, wbuf.at[mp], loc.at[0])
    own_w.start()
    later = [
        pltpu.make_async_copy(src, dst, loc.at[1 + j])
        for j, (src, dst) in enumerate(((qkv_h, qkv), (out_h, out_w), (up_h, up), (down_h, down)))
    ]
    for c in later:
        c.start()
    pos[...] = jnp.transpose(pos_t[...].astype(jnp.float32)).astype(jnp.bfloat16)
    pbuf[mp] = pos[pl.ds(pl.multiple_of(mp * quarter, quarter), quarter)]

    count = selected.shape[0]

    def row_of(i):
        return owner_row[selected[i]]

    def pick(learner):
        def body(i, found):
            row = row_of(i)
            hit = (lax.div(dest_slot[i], per) == learner) & (lax.div(row, stored) == dp)
            return jnp.where(hit, lax.rem(row, stored), found)
        return lax.fori_loop(0, count, body, jnp.int32(0), unroll=count <= 16)

    def sender(slot):
        def body(i, found):
            return jnp.where(dest_slot[i] == slot, lax.div(row_of(i), stored), found)
        return lax.fori_loop(0, count, body, jnp.int32(0), unroll=count <= 16)

    recv[dp] = cand[pick(dp)]

    @pl.loop(1, n_dp)
    def _(k):
        learner = lax.rem(dp + n_dp - k, n_dp)
        send[learner] = cand[pick(learner)]

    pl.semaphore_wait(barrier, 3 + n_dp - 1)

    def remote(src, dst, ss, rs, where):
        return pltpu.make_async_remote_copy(
            src_ref=src, dst_ref=dst, send_sem=ss, recv_sem=rs, device_id=where, device_id_type=MESH
        )

    mine = pl.ds(pl.multiple_of(lax.rem(dp, 2) * half, half), half)
    w_side = remote(pw.at[mine], wbuf.at[mp, mine], w_s.at[0], w_r.at[0], (dp, side))
    w_across = remote(pw.at[mine], wbuf.at[mp, mine], w_s.at[1], w_r.at[1], (dp, across))
    w_across.start()
    w_side.start()
    p_copies = []
    for j, other in enumerate((side, across, corner)):
        c = remote(pos.at[pl.ds(other * quarter, quarter)], pbuf.at[mp], p_s.at[j], p_r.at[j], (dp, other))
        c.start()
        p_copies.append(c)

    @pl.loop(1, n_dp)
    def _(k):
        learner = lax.rem(dp + n_dp - k, n_dp)
        remote(send.at[learner], recv.at[dp], route_s.at[learner], route_r.at[dp], (learner, mp)).start()

    for c in p_copies:
        c.wait()
    for g in range(n_mp):
        act[:, g * feats:(g + 1) * feats] = jnp.concatenate([pbuf[g].astype(jnp.float32)] * per, axis=0)
    w_across.wait_recv()
    w_fwd = remote(wbuf.at[across, mine], wbuf.at[across, mine], w_s.at[2], w_r.at[2], (dp, side))
    w_fwd.start()
    d_copies = []

    def to_twin(j, block):
        c = remote(wbuf.at[block, mine], wbuf.at[block, mine], d_s.at[j], d_r.at[j], (twin, mp))
        c.start()
        d_copies.append(c)

    to_twin(0, across)
    w_side.wait_recv()
    to_twin(1, side)
    w_fwd.wait_recv()
    to_twin(2, corner)

    @pl.loop(1, n_dp)
    def _(k):
        peer = lax.rem(dp + k, n_dp)
        remote(send.at[peer], recv.at[peer], route_s.at[peer], route_r.at[peer], (peer, mp)).wait()

    own_w.wait()
    for e in range(per):
        xbuf[e * quarter:(e + 1) * quarter] = recv[sender(dp * per + e)]
    for c in d_copies:
        c.wait()
    for c in (w_side, w_across, w_fwd):
        c.wait_send()

    prod = dot_t(xbuf[...], wbuf[...].reshape(n_mp * feats, width))
    act[...] = (prod + act[...]).astype(jnp.bfloat16).astype(jnp.float32)

    def gather_start(buf, base, e):
        cs = []
        for j, other in enumerate((across, side)):
            c = remote(buf.at[e, mp], buf.at[e, mp], ag_s.at[base + j], ag_r.at[base + j], (dp, other))
            c.start()
            cs.append(c)
        return cs

    def gather_forward(buf, base, e, cs):
        cs[0].wait_recv()
        c = remote(buf.at[e, across], buf.at[e, across], ag_s.at[base + 2], ag_r.at[base + 2], (dp, side))
        c.start()
        cs.append(c)

    def gather_end(cs):
        cs[1].wait_recv()
        cs[2].wait_recv()
        for c in cs:
            c.wait_send()

    def sum_start(part, ra, base, e):
        cs = []
        for j, block in enumerate((corner, side)):
            c = remote(part.at[e, block], ra.at[e, j], rs_s.at[base + j], rs_r.at[base + j], (dp, side))
            c.start()
            cs.append(c)
        return cs

    def sum_merge(part, ra, rm, rb, base, e, cs):
        cs[0].wait_recv()
        rm[e] = (part[e, across].astype(jnp.float32) + ra[e, 0].astype(jnp.float32)).astype(jnp.bfloat16)
        c = remote(rm.at[e], rb.at[e], rs_s.at[base + 2], rs_r.at[base + 2], (dp, across))
        c.start()
        cs.append(c)

    def sum_end(part, ra, rb, e, cs):
        cs[1].wait_recv()
        cs[2].wait_recv()
        for c in cs:
            c.wait_send()
        return part[e, mp].astype(jnp.float32) + ra[e, 1].astype(jnp.float32) + rb[e].astype(jnp.float32)

    def rows(e):
        return pl.ds(e * quarter, quarter)

    g1 = gain1[...].astype(jnp.float32).reshape(1, width)
    g2 = gain2[...].astype(jnp.float32).reshape(1, width)
    every = range(per)
    gathers = []
    for e in every:
        ag1[e, mp] = norm_rows(act[rows(e)], g1).astype(jnp.bfloat16)
        gathers.append(gather_start(ag1, 3 * e, e))
    for e in every:
        gather_forward(ag1, 3 * e, e, gathers[e])

    tokens = n_mp * quarter
    sums = []
    for e in every:
        gather_end(gathers[e])
        if e == 0:
            later[0].wait()
            later[1].wait()
        normed = ag1[e].reshape(tokens, width)
        qkv_all = dot_t(normed, qkv[...].reshape(3 * feats, width)).astype(jnp.bfloat16)
        q = qkv_all[:, :feats] * jnp.bfloat16(HEAD_DIM ** (-0.5))
        k = qkv_all[:, feats:2 * feats]
        v = qkv_all[:, 2 * feats:]
        for h in range(feats // HEAD_DIM):
            cut = slice(h * HEAD_DIM, (h + 1) * HEAD_DIM)
            s = dot_t(q[:, cut], k[:, cut])
            p = jnp.exp(s - jnp.max(s, axis=-1, keepdims=True))
            total = jnp.sum(p, axis=-1, keepdims=True)
            ctx[:, cut] = (dot(p.astype(jnp.bfloat16), v[:, cut]) / total).astype(jnp.bfloat16)
        part1[e] = dot(ctx[...], out_w[...]).astype(jnp.bfloat16).reshape(n_mp, quarter, width)
        sums.append(sum_start(part1, ra1, 3 * e, e))
    for e in every:
        sum_merge(part1, ra1, rm1, rb1, 3 * e, e, sums[e])
    gathers = []
    for e in every:
        value = act[rows(e)] + sum_end(part1, ra1, rb1, e, sums[e])
        after[rows(e)] = value
        ag2[e, mp] = norm_rows(value, g2).astype(jnp.bfloat16)
        gathers.append(gather_start(ag2, 3 * (per + e), e))
    for e in every:
        gather_forward(ag2, 3 * (per + e), e, gathers[e])
    sums = []
    for e in every:
        gather_end(gathers[e])
        if e == 0:
            later[2].wait()
            later[3].wait()
        x = dot(ag2[e].reshape(tokens, width), up[...])
        hidden = (0.5 * x * (1.0 + lax.erf(x * 0.7071067811865476))).astype(jnp.bfloat16)
        part2[e] = dot(hidden, down[...]).astype(jnp.bfloat16).reshape(n_mp, quarter, width)
        sums.append(sum_start(part2, ra2, 3 * (per + e), e))
    for e in every:
        sum_merge(part2, ra2, rm2, rb2, 3 * (per + e), e, sums[e])
    for e in every:
        out[e] = (after[rows(e)] + sum_end(part2, ra2, rb2, e, sums[e])).astype(jnp.bfloat16)


def solution(mesh):
    n_dp, n_mp = mesh.shape["dp"], mesh.shape["mp"]

    def local(
        candidates, owner_row, selected, dest_slot, patch_weight, positions,
        qkv_weight, out_weight, attn_gain, mlp_gain, up_weight, down_weight,
    ):
        stored, quarter, width = candidates.shape
        per = selected.shape[0] // n_dp
        feats = patch_weight.shape[1]
        qkv = jnp.transpose(qkv_weight, (1, 2, 0))
        vm = pl.BlockSpec(memory_space=pltpu.VMEM)
        sm = pl.BlockSpec(memory_space=pltpu.SMEM)
        bf, f32 = jnp.bfloat16, jnp.float32
        blocks = pltpu.VMEM((per, n_mp, quarter, width), bf)
        pair = pltpu.VMEM((per, 2, quarter, width), bf)
        one = pltpu.VMEM((per, quarter, width), bf)
        dma = pltpu.SemaphoreType.DMA
        return pl.pallas_call(
            functools.partial(kernel, n_dp, n_mp, stored, per),
            out_shape=jax.ShapeDtypeStruct((per, quarter, width), bf),
            in_specs=[sm] * 3 + [vm] * 5 + [pl.BlockSpec(memory_space=pl.ANY)] * 4,
            out_specs=vm,
            scratch_shapes=[
                pltpu.VMEM(qkv.shape, bf), pltpu.VMEM(out_weight.shape, bf),
                pltpu.VMEM(up_weight.shape, bf), pltpu.VMEM(down_weight.shape, bf),
                pltpu.VMEM(positions.shape, bf),
                pltpu.VMEM((n_dp, quarter, width), bf),
                pltpu.VMEM((n_dp, quarter, width), bf),
                pltpu.VMEM((n_mp, feats, width), bf),
                pltpu.VMEM((n_mp, quarter, feats), bf),
                pltpu.VMEM((per * quarter, width), bf),
                pltpu.VMEM((per * quarter, n_mp * feats), f32),
                pltpu.VMEM((per * quarter, n_mp * feats), f32),
                pltpu.VMEM((n_mp * quarter, feats), bf),
                blocks, blocks, pair, one, one,
                blocks, blocks, pair, one, one,
                dma((n_dp,)), dma((n_dp,)),
                dma((3,)), dma((3,)), dma((3,)), dma((3,)), dma((3,)), dma((3,)),
                dma((6 * per,)), dma((6 * per,)), dma((6 * per,)), dma((6 * per,)),
                dma((5,)),
            ],
            compiler_params=pltpu.CompilerParams(
                collective_id=0, has_side_effects=True, vmem_limit_bytes=60000 * 1024
            ),
        )(
            owner_row, selected, dest_slot, candidates, patch_weight.T, positions.T,
            attn_gain, mlp_gain, qkv, out_weight, up_weight, down_weight,
        )

    return jax.shard_map(
        local,
        mesh=mesh,
        in_specs=(
            P("dp", "mp", None), P(), P(), P(), P(None, "mp"), P(None, "mp"), P(None, None, "mp"),
            P("mp", None), P(), P(), P(None, "mp"), P("mp", None),
        ),
        out_specs=P("dp", "mp", None),
        check_vma=False,
    )
```

```python
import functools

import jax
import jax.numpy as jnp
from jax import lax
from jax.experimental import pallas as pl
from jax.experimental.pallas import tpu as pltpu
from jax.sharding import PartitionSpec as P

HEAD_DIM = 64
MESH = pl.DeviceIdType.MESH


def norm_rows(values, gain):
    average = jnp.mean(values, axis=-1, keepdims=True)
    centred = values - average
    variance = jnp.mean(centred * centred, axis=-1, keepdims=True)
    return centred * lax.rsqrt(variance + 1e-06) * gain


def dot(a, b):
    return jnp.dot(a, b, preferred_element_type=jnp.float32)


def dot_t(a, b):
    return lax.dot_general(a, b, (((1,), (1,)), ((), ())), preferred_element_type=jnp.float32)


def kernel(
    n_dp, n_mp, stored, per,
    owner_row, selected, dest_slot,
    cand_h, pw, pos_t, gain1, gain2, qkv_h, out_h, up_h, down_h,
    out,
    cand, qkv, out_w, up, down, pos,
    send, recv, wbuf, pbuf, xbuf, act, after, ctx, ag1, part1, ra1, rm1, rb1, ag2, part2, ra2, rm2, rb2,
    route_s, route_r, w_s, w_r, d_s, d_r, p_s, p_r, ag_s, ag_r, rs_s, rs_r, loc,
):
    dp = lax.axis_index("dp")
    mp = lax.axis_index("mp")
    quarter, width = cand.shape[1], cand.shape[2]
    feats = pw.shape[0]
    half = feats // 2
    side = mp + 1 - 2 * lax.rem(mp, 2)
    across = lax.rem(mp + n_mp // 2, n_mp)
    corner = n_mp - 1 - mp
    twin = dp + 1 - 2 * lax.rem(dp, 2)

    barrier = pltpu.get_barrier_semaphore()
    for other in (side, across, corner):
        pl.semaphore_signal(barrier, inc=1, device_id=(dp, other), device_id_type=MESH)

    @pl.loop(1, n_dp)
    def _(k):
        pl.semaphore_signal(barrier, inc=1, device_id=(lax.rem(dp + k, n_dp), mp), device_id_type=MESH)

    own_c = pltpu.make_async_copy(cand_h, cand, loc.at[5])
    own_c.start()
    own_w = pltpu.make_async_copy(pw, wbuf.at[mp], loc.at[0])
    own_w.start()
    pos[...] = jnp.transpose(pos_t[...].astype(jnp.float32)).astype(jnp.bfloat16)
    pbuf[mp] = pos[pl.ds(pl.multiple_of(mp * quarter, quarter), quarter)]
    later = [
        pltpu.make_async_copy(src, dst, loc.at[1 + j])
        for j, (src, dst) in enumerate(((qkv_h, qkv), (out_h, out_w), (up_h, up), (down_h, down)))
    ]

    pl.semaphore_wait(barrier, 3 + n_dp - 1)

    def remote(src, dst, ss, rs, where):
        return pltpu.make_async_remote_copy(
            src_ref=src, dst_ref=dst, send_sem=ss, recv_sem=rs, device_id=where, device_id_type=MESH
        )

    mine = pl.ds(pl.multiple_of(lax.rem(dp, 2) * half, half), half)
    w_side = remote(pw.at[mine], wbuf.at[mp, mine], w_s.at[0], w_r.at[0], (dp, side))
    w_across = remote(pw.at[mine], wbuf.at[mp, mine], w_s.at[1], w_r.at[1], (dp, across))
    w_across.start()
    w_side.start()
    p_copies = []
    for j, other in enumerate((side, across, corner)):
        c = remote(pos.at[pl.ds(other * quarter, quarter)], pbuf.at[mp], p_s.at[j], p_r.at[j], (dp, other))
        c.start()
        p_copies.append(c)

    count = selected.shape[0]
    short = count <= 16

    def route(i):
        row = owner_row[selected[i]]
        slot = dest_slot[i]
        owner = lax.div(row, stored)
        return slot, owner, jnp.where(owner == dp, lax.div(slot, per), -1), lax.rem(row, stored)

    routes = [route(i) for i in range(count)] if short else []

    def choose(key, value, wanted):
        if short:
            found = jnp.int32(0)
            for entry in routes:
                found = jnp.where(entry[key] == wanted, entry[value], found)
            return found

        def body(i, found):
            entry = route(i)
            return jnp.where(entry[key] == wanted, entry[value], found)
        return lax.fori_loop(0, count, body, jnp.int32(0))

    def pass_on(k):
        learner = lax.rem(dp + n_dp - k, n_dp)
        send[learner] = cand[choose(2, 3, learner)]
        remote(send.at[learner], recv.at[dp], route_s.at[learner], route_r.at[dp], (learner, mp)).start()

    own_c.wait()
    if short:
        for k in range(1, n_dp):
            pass_on(k)
    else:
        pl.loop(1, n_dp)(pass_on)
    recv[dp] = cand[choose(2, 3, dp)]
    for c in later:
        c.start()
    senders = [choose(0, 1, dp * per + e) for e in range(per)]

    w_across.wait_recv()
    w_fwd = remote(wbuf.at[across, mine], wbuf.at[across, mine], w_s.at[2], w_r.at[2], (dp, side))
    w_fwd.start()
    d_copies = []

    def to_twin(j, block):
        c = remote(wbuf.at[block, mine], wbuf.at[block, mine], d_s.at[j], d_r.at[j], (twin, mp))
        c.start()
        d_copies.append(c)

    to_twin(0, across)
    w_side.wait_recv()
    to_twin(1, side)
    for c in p_copies:
        c.wait()
    for g in range(n_mp):
        act[:, g * feats:(g + 1) * feats] = jnp.concatenate([pbuf[g].astype(jnp.float32)] * per, axis=0)
    w_fwd.wait_recv()
    to_twin(2, corner)

    @pl.loop(1, n_dp)
    def _(k):
        peer = lax.rem(dp + k, n_dp)
        remote(send.at[peer], recv.at[peer], route_s.at[peer], route_r.at[peer], (peer, mp)).wait()

    own_w.wait()
    for e in range(per):
        xbuf[e * quarter:(e + 1) * quarter] = recv[senders[e]]
    for c in d_copies:
        c.wait()
    for c in (w_side, w_across, w_fwd):
        c.wait_send()

    prod = dot_t(xbuf[...], wbuf[...].reshape(n_mp * feats, width))
    act[...] = (prod + act[...]).astype(jnp.bfloat16).astype(jnp.float32)

    def gather_start(buf, base, e):
        cs = []
        for j, other in enumerate((across, side)):
            c = remote(buf.at[e, mp], buf.at[e, mp], ag_s.at[base + j], ag_r.at[base + j], (dp, other))
            c.start()
            cs.append(c)
        return cs

    def gather_forward(buf, base, e, cs):
        cs[0].wait_recv()
        c = remote(buf.at[e, across], buf.at[e, across], ag_s.at[base + 2], ag_r.at[base + 2], (dp, side))
        c.start()
        cs.append(c)

    def gather_end(cs):
        cs[1].wait_recv()
        cs[2].wait_recv()
        for c in cs:
            c.wait_send()

    def sum_start(part, ra, base, e):
        cs = []
        for j, block in enumerate((corner, side)):
            c = remote(part.at[e, block], ra.at[e, j], rs_s.at[base + j], rs_r.at[base + j], (dp, side))
            c.start()
            cs.append(c)
        return cs

    def sum_merge(part, ra, rm, rb, base, e, cs):
        cs[0].wait_recv()
        rm[e] = (part[e, across].astype(jnp.float32) + ra[e, 0].astype(jnp.float32)).astype(jnp.bfloat16)
        c = remote(rm.at[e], rb.at[e], rs_s.at[base + 2], rs_r.at[base + 2], (dp, across))
        c.start()
        cs.append(c)

    def sum_end(part, ra, rb, e, cs):
        cs[1].wait_recv()
        cs[2].wait_recv()
        for c in cs:
            c.wait_send()
        return part[e, mp].astype(jnp.float32) + ra[e, 1].astype(jnp.float32) + rb[e].astype(jnp.float32)

    def rows(e):
        return pl.ds(e * quarter, quarter)

    g1 = gain1[...].astype(jnp.float32).reshape(1, width)
    g2 = gain2[...].astype(jnp.float32).reshape(1, width)
    every = range(per)
    gathers = []
    for e in every:
        ag1[e, mp] = norm_rows(act[rows(e)], g1).astype(jnp.bfloat16)
        gathers.append(gather_start(ag1, 3 * e, e))
    for e in every:
        gather_forward(ag1, 3 * e, e, gathers[e])

    tokens = n_mp * quarter
    sums = []
    for e in every:
        gather_end(gathers[e])
        if e == 0:
            later[0].wait()
            later[1].wait()
        normed = ag1[e].reshape(tokens, width)
        qkv_all = dot_t(normed, qkv[...].reshape(3 * feats, width)).astype(jnp.bfloat16)
        q = qkv_all[:, :feats] * jnp.bfloat16(HEAD_DIM ** (-0.5))
        k = qkv_all[:, feats:2 * feats]
        v = qkv_all[:, 2 * feats:]
        for h in range(feats // HEAD_DIM):
            cut = slice(h * HEAD_DIM, (h + 1) * HEAD_DIM)
            s = dot_t(q[:, cut], k[:, cut])
            p = jnp.exp(s - jnp.max(s, axis=-1, keepdims=True))
            total = jnp.sum(p, axis=-1, keepdims=True)
            ctx[:, cut] = (dot(p.astype(jnp.bfloat16), v[:, cut]) / total).astype(jnp.bfloat16)
        part1[e] = dot(ctx[...], out_w[...]).astype(jnp.bfloat16).reshape(n_mp, quarter, width)
        sums.append(sum_start(part1, ra1, 3 * e, e))
    for e in every:
        sum_merge(part1, ra1, rm1, rb1, 3 * e, e, sums[e])
    gathers = []
    for e in every:
        value = act[rows(e)] + sum_end(part1, ra1, rb1, e, sums[e])
        after[rows(e)] = value
        ag2[e, mp] = norm_rows(value, g2).astype(jnp.bfloat16)
        gathers.append(gather_start(ag2, 3 * (per + e), e))
    for e in every:
        gather_forward(ag2, 3 * (per + e), e, gathers[e])
    sums = []
    for e in every:
        gather_end(gathers[e])
        if e == 0:
            later[2].wait()
            later[3].wait()
        x = dot(ag2[e].reshape(tokens, width), up[...])
        hidden = (0.5 * x * (1.0 + lax.erf(x * 0.7071067811865476))).astype(jnp.bfloat16)
        part2[e] = dot(hidden, down[...]).astype(jnp.bfloat16).reshape(n_mp, quarter, width)
        sums.append(sum_start(part2, ra2, 3 * (per + e), e))
    for e in every:
        sum_merge(part2, ra2, rm2, rb2, 3 * (per + e), e, sums[e])
    for e in every:
        out[e] = (after[rows(e)] + sum_end(part2, ra2, rb2, e, sums[e])).astype(jnp.bfloat16)


def solution(mesh):
    n_dp, n_mp = mesh.shape["dp"], mesh.shape["mp"]

    def local(
        candidates, owner_row, selected, dest_slot, patch_weight, positions,
        qkv_weight, out_weight, attn_gain, mlp_gain, up_weight, down_weight,
    ):
        stored, quarter, width = candidates.shape
        per = selected.shape[0] // n_dp
        feats = patch_weight.shape[1]
        qkv = jnp.transpose(qkv_weight, (1, 2, 0))
        vm = pl.BlockSpec(memory_space=pltpu.VMEM)
        hb = pl.BlockSpec(memory_space=pl.ANY)
        sm = pl.BlockSpec(memory_space=pltpu.SMEM)
        bf, f32 = jnp.bfloat16, jnp.float32
        blocks = pltpu.VMEM((per, n_mp, quarter, width), bf)
        pair = pltpu.VMEM((per, 2, quarter, width), bf)
        one = pltpu.VMEM((per, quarter, width), bf)
        dma = pltpu.SemaphoreType.DMA
        return pl.pallas_call(
            functools.partial(kernel, n_dp, n_mp, stored, per),
            out_shape=jax.ShapeDtypeStruct((per, quarter, width), bf),
            in_specs=[sm] * 3 + [hb] * 2 + [vm] * 3 + [hb] * 4,
            out_specs=vm,
            scratch_shapes=[
                pltpu.VMEM(candidates.shape, bf), pltpu.VMEM(qkv.shape, bf), pltpu.VMEM(out_weight.shape, bf),
                pltpu.VMEM(up_weight.shape, bf), pltpu.VMEM(down_weight.shape, bf),
                pltpu.VMEM(positions.shape, bf),
                pltpu.VMEM((n_dp, quarter, width), bf),
                pltpu.VMEM((n_dp, quarter, width), bf),
                pltpu.VMEM((n_mp, feats, width), bf),
                pltpu.VMEM((n_mp, quarter, feats), bf),
                pltpu.VMEM((per * quarter, width), bf),
                pltpu.VMEM((per * quarter, n_mp * feats), f32),
                pltpu.VMEM((per * quarter, n_mp * feats), f32),
                pltpu.VMEM((n_mp * quarter, feats), bf),
                blocks, blocks, pair, one, one,
                blocks, blocks, pair, one, one,
                dma((n_dp,)), dma((n_dp,)),
                dma((3,)), dma((3,)), dma((3,)), dma((3,)), dma((3,)), dma((3,)),
                dma((6 * per,)), dma((6 * per,)), dma((6 * per,)), dma((6 * per,)),
                dma((6,)),
            ],
            compiler_params=pltpu.CompilerParams(
                collective_id=0, has_side_effects=True, vmem_limit_bytes=60000 * 1024
            ),
        )(
            owner_row, selected, dest_slot, candidates, patch_weight.T, positions.T,
            attn_gain, mlp_gain, qkv, out_weight, up_weight, down_weight,
        )

    return jax.shard_map(
        local,
        mesh=mesh,
        in_specs=(
            P("dp", "mp", None), P(), P(), P(), P(None, "mp"), P(None, "mp"), P(None, None, "mp"),
            P("mp", None), P(), P(), P(None, "mp"), P("mp", None),
        ),
        out_specs=P("dp", "mp", None),
        check_vma=False,
    )
```

```python
import functools

import jax
import jax.numpy as jnp
from jax import lax
from jax.experimental import pallas as pl
from jax.experimental.pallas import tpu as pltpu
from jax.sharding import PartitionSpec as P

HEAD_DIM = 64
MESH = pl.DeviceIdType.MESH


def norm_rows(values, gain):
    average = jnp.mean(values, axis=-1, keepdims=True)
    centred = values - average
    variance = jnp.mean(centred * centred, axis=-1, keepdims=True)
    return centred * lax.rsqrt(variance + 1e-06) * gain


def dot(a, b):
    return jnp.dot(a, b, preferred_element_type=jnp.float32)


def dot_t(a, b):
    return lax.dot_general(a, b, (((1,), (1,)), ((), ())), preferred_element_type=jnp.float32)


def kernel(
    n_dp, n_mp, stored, per,
    owner_row, selected, dest_slot,
    cand_h, pw, pos_t, gain1, gain2, qkv_h, out_h, up_h, down_h,
    out,
    cand, qkv, out_w, up, down, pos,
    send, recv, wbuf, pbuf, xbuf, act, after, ctx, ag1, part1, ra1, rm1, rb1, ag2, part2, ra2, rm2, rb2,
    route_s, route_r, w_s, w_r, d_s, d_r, p_s, p_r, ag_s, ag_r, rs_s, rs_r, loc,
):
    dp = lax.axis_index("dp")
    mp = lax.axis_index("mp")
    quarter, width = cand.shape[1], cand.shape[2]
    feats = pw.shape[0]
    half = feats // 2
    side = mp + 1 - 2 * lax.rem(mp, 2)
    across = lax.rem(mp + n_mp // 2, n_mp)
    corner = n_mp - 1 - mp
    twin = dp + 1 - 2 * lax.rem(dp, 2)

    barrier = pltpu.get_barrier_semaphore()
    for other in (side, across, corner):
        pl.semaphore_signal(barrier, inc=1, device_id=(dp, other), device_id_type=MESH)

    @pl.loop(1, n_dp)
    def _(k):
        pl.semaphore_signal(barrier, inc=1, device_id=(lax.rem(dp + k, n_dp), mp), device_id_type=MESH)

    own_c = pltpu.make_async_copy(cand_h, cand, loc.at[5])
    own_c.start()
    own_w = pltpu.make_async_copy(pw, wbuf.at[mp], loc.at[0])
    own_w.start()
    pos[...] = jnp.transpose(pos_t[...].astype(jnp.float32)).astype(jnp.bfloat16)
    pbuf[mp] = pos[pl.ds(pl.multiple_of(mp * quarter, quarter), quarter)]
    later = [
        pltpu.make_async_copy(src, dst, loc.at[1 + j])
        for j, (src, dst) in enumerate(((qkv_h, qkv), (out_h, out_w), (up_h, up), (down_h, down)))
    ]

    pl.semaphore_wait(barrier, 3 + n_dp - 1)

    def remote(src, dst, ss, rs, where):
        return pltpu.make_async_remote_copy(
            src_ref=src, dst_ref=dst, send_sem=ss, recv_sem=rs, device_id=where, device_id_type=MESH
        )

    mine = pl.ds(pl.multiple_of(lax.rem(dp, 2) * half, half), half)
    w_side = remote(pw.at[mine], wbuf.at[mp, mine], w_s.at[0], w_r.at[0], (dp, side))
    w_across = remote(pw.at[mine], wbuf.at[mp, mine], w_s.at[1], w_r.at[1], (dp, across))
    w_across.start()
    w_side.start()
    p_copies = []
    for j, other in enumerate((side, across, corner)):
        c = remote(pos.at[pl.ds(other * quarter, quarter)], pbuf.at[mp], p_s.at[j], p_r.at[j], (dp, other))
        c.start()
        p_copies.append(c)

    count = selected.shape[0]
    short = count <= 16

    def route(i):
        row = owner_row[selected[i]]
        slot = dest_slot[i]
        owner = lax.div(row, stored)
        return slot, owner, jnp.where(owner == dp, lax.div(slot, per), -1), lax.rem(row, stored)

    routes = [route(i) for i in range(count)] if short else []

    def choose(key, value, wanted):
        if short:
            found = jnp.int32(0)
            for entry in routes:
                found = jnp.where(entry[key] == wanted, entry[value], found)
            return found

        def body(i, found):
            entry = route(i)
            return jnp.where(entry[key] == wanted, entry[value], found)
        return lax.fori_loop(0, count, body, jnp.int32(0))

    def pass_on(k):
        learner = lax.rem(dp + n_dp - k, n_dp)
        send[learner] = cand[choose(2, 3, learner)]
        remote(send.at[learner], recv.at[dp], route_s.at[learner], route_r.at[dp], (learner, mp)).start()

    own_c.wait()
    if short:
        for k in range(1, n_dp):
            pass_on(k)
    else:
        pl.loop(1, n_dp)(pass_on)
    recv[dp] = cand[choose(2, 3, dp)]
    for c in later:
        c.start()
    senders = [choose(0, 1, dp * per + e) for e in range(per)]

    w_across.wait_recv()
    w_fwd = remote(wbuf.at[across, mine], wbuf.at[across, mine], w_s.at[2], w_r.at[2], (dp, side))
    w_fwd.start()
    d_copies = []

    def to_twin(j, block):
        c = remote(wbuf.at[block, mine], wbuf.at[block, mine], d_s.at[j], d_r.at[j], (twin, mp))
        c.start()
        d_copies.append(c)

    to_twin(0, across)
    w_side.wait_recv()
    to_twin(1, side)
    for c in p_copies:
        c.wait()
    for g in range(n_mp):
        act[:, g * feats:(g + 1) * feats] = jnp.concatenate([pbuf[g].astype(jnp.float32)] * per, axis=0)
    w_fwd.wait_recv()
    to_twin(2, corner)

    @pl.loop(1, n_dp)
    def _(k):
        peer = lax.rem(dp + k, n_dp)
        remote(send.at[peer], recv.at[peer], route_s.at[peer], route_r.at[peer], (peer, mp)).wait()

    own_w.wait()
    for e in range(per):
        xbuf[e * quarter:(e + 1) * quarter] = recv[senders[e]]
    for c in d_copies:
        c.wait()
    for c in (w_side, w_across, w_fwd):
        c.wait_send()

    prod = dot_t(xbuf[...], wbuf[...].reshape(n_mp * feats, width))
    act[...] = (prod + act[...]).astype(jnp.bfloat16).astype(jnp.float32)

    def gather_send(buf, base, e, j, cs):
        other = (across, side)[j]
        c = remote(buf.at[e, mp], buf.at[e, mp], ag_s.at[base + j], ag_r.at[base + j], (dp, other))
        c.start()
        cs.append(c)

    def gather_start(buf, base, e):
        cs = []
        gather_send(buf, base, e, 0, cs)
        if e == 0:
            gather_send(buf, base, e, 1, cs)
        return cs

    def gather_forward(buf, base, e, cs):
        cs[0].wait_recv()
        c = remote(buf.at[e, across], buf.at[e, across], ag_s.at[base + 2], ag_r.at[base + 2], (dp, side))
        c.start()
        cs.append(c)

    def gather_end(cs):
        cs[1].wait_recv()
        cs[2].wait_recv()
        for c in cs:
            c.wait_send()

    def sum_start(part, ra, base, e):
        cs = []
        for j, block in enumerate((corner, side)):
            c = remote(part.at[e, block], ra.at[e, j], rs_s.at[base + j], rs_r.at[base + j], (dp, side))
            c.start()
            cs.append(c)
        return cs

    def sum_merge(part, ra, rm, rb, base, e, cs):
        cs[0].wait_recv()
        rm[e] = (part[e, across].astype(jnp.float32) + ra[e, 0].astype(jnp.float32)).astype(jnp.bfloat16)
        c = remote(rm.at[e], rb.at[e], rs_s.at[base + 2], rs_r.at[base + 2], (dp, across))
        c.start()
        cs.append(c)

    def sum_end(part, ra, rb, e, cs):
        cs[1].wait_recv()
        cs[2].wait_recv()
        for c in cs:
            c.wait_send()
        return part[e, mp].astype(jnp.float32) + ra[e, 1].astype(jnp.float32) + rb[e].astype(jnp.float32)

    def rows(e):
        return pl.ds(e * quarter, quarter)

    g1 = gain1[...].astype(jnp.float32).reshape(1, width)
    g2 = gain2[...].astype(jnp.float32).reshape(1, width)
    every = range(per)
    gathers = []
    for e in every:
        ag1[e, mp] = norm_rows(act[rows(e)], g1).astype(jnp.bfloat16)
        gathers.append(gather_start(ag1, 3 * e, e))
    for e in every:
        gather_forward(ag1, 3 * e, e, gathers[e])
        if e + 1 < per:
            gather_send(ag1, 3 * (e + 1), e + 1, 1, gathers[e + 1])

    tokens = n_mp * quarter
    sums = []
    for e in every:
        gather_end(gathers[e])
        if e == 0:
            later[0].wait()
            later[1].wait()
        normed = ag1[e].reshape(tokens, width)
        qkv_all = dot_t(normed, qkv[...].reshape(3 * feats, width)).astype(jnp.bfloat16)
        q = qkv_all[:, :feats] * jnp.bfloat16(HEAD_DIM ** (-0.5))
        k = qkv_all[:, feats:2 * feats]
        v = qkv_all[:, 2 * feats:]
        for h in range(feats // HEAD_DIM):
            cut = slice(h * HEAD_DIM, (h + 1) * HEAD_DIM)
            s = dot_t(q[:, cut], k[:, cut])
            p = jnp.exp(s - jnp.max(s, axis=-1, keepdims=True))
            total = jnp.sum(p, axis=-1, keepdims=True)
            ctx[:, cut] = (dot(p.astype(jnp.bfloat16), v[:, cut]) / total).astype(jnp.bfloat16)
        part1[e] = dot(ctx[...], out_w[...]).astype(jnp.bfloat16).reshape(n_mp, quarter, width)
        sums.append(sum_start(part1, ra1, 3 * e, e))
    for e in every:
        sum_merge(part1, ra1, rm1, rb1, 3 * e, e, sums[e])
    gathers = []
    for e in every:
        value = act[rows(e)] + sum_end(part1, ra1, rb1, e, sums[e])
        after[rows(e)] = value
        ag2[e, mp] = norm_rows(value, g2).astype(jnp.bfloat16)
        gathers.append(gather_start(ag2, 3 * (per + e), e))
    for e in every:
        gather_forward(ag2, 3 * (per + e), e, gathers[e])
        if e + 1 < per:
            gather_send(ag2, 3 * (per + e + 1), e + 1, 1, gathers[e + 1])
    sums = []
    for e in every:
        gather_end(gathers[e])
        if e == 0:
            later[2].wait()
            later[3].wait()
        x = dot(ag2[e].reshape(tokens, width), up[...])
        hidden = (0.5 * x * (1.0 + lax.erf(x * 0.7071067811865476))).astype(jnp.bfloat16)
        part2[e] = dot(hidden, down[...]).astype(jnp.bfloat16).reshape(n_mp, quarter, width)
        sums.append(sum_start(part2, ra2, 3 * (per + e), e))
    for e in every:
        sum_merge(part2, ra2, rm2, rb2, 3 * (per + e), e, sums[e])
    for e in every:
        out[e] = (after[rows(e)] + sum_end(part2, ra2, rb2, e, sums[e])).astype(jnp.bfloat16)


def solution(mesh):
    n_dp, n_mp = mesh.shape["dp"], mesh.shape["mp"]

    def local(
        candidates, owner_row, selected, dest_slot, patch_weight, positions,
        qkv_weight, out_weight, attn_gain, mlp_gain, up_weight, down_weight,
    ):
        stored, quarter, width = candidates.shape
        per = selected.shape[0] // n_dp
        feats = patch_weight.shape[1]
        qkv = jnp.transpose(qkv_weight, (1, 2, 0))
        vm = pl.BlockSpec(memory_space=pltpu.VMEM)
        hb = pl.BlockSpec(memory_space=pl.ANY)
        sm = pl.BlockSpec(memory_space=pltpu.SMEM)
        bf, f32 = jnp.bfloat16, jnp.float32
        blocks = pltpu.VMEM((per, n_mp, quarter, width), bf)
        pair = pltpu.VMEM((per, 2, quarter, width), bf)
        one = pltpu.VMEM((per, quarter, width), bf)
        dma = pltpu.SemaphoreType.DMA
        return pl.pallas_call(
            functools.partial(kernel, n_dp, n_mp, stored, per),
            out_shape=jax.ShapeDtypeStruct((per, quarter, width), bf),
            in_specs=[sm] * 3 + [hb] * 2 + [vm] * 3 + [hb] * 4,
            out_specs=vm,
            scratch_shapes=[
                pltpu.VMEM(candidates.shape, bf), pltpu.VMEM(qkv.shape, bf), pltpu.VMEM(out_weight.shape, bf),
                pltpu.VMEM(up_weight.shape, bf), pltpu.VMEM(down_weight.shape, bf),
                pltpu.VMEM(positions.shape, bf),
                pltpu.VMEM((n_dp, quarter, width), bf),
                pltpu.VMEM((n_dp, quarter, width), bf),
                pltpu.VMEM((n_mp, feats, width), bf),
                pltpu.VMEM((n_mp, quarter, feats), bf),
                pltpu.VMEM((per * quarter, width), bf),
                pltpu.VMEM((per * quarter, n_mp * feats), f32),
                pltpu.VMEM((per * quarter, n_mp * feats), f32),
                pltpu.VMEM((n_mp * quarter, feats), bf),
                blocks, blocks, pair, one, one,
                blocks, blocks, pair, one, one,
                dma((n_dp,)), dma((n_dp,)),
                dma((3,)), dma((3,)), dma((3,)), dma((3,)), dma((3,)), dma((3,)),
                dma((6 * per,)), dma((6 * per,)), dma((6 * per,)), dma((6 * per,)),
                dma((6,)),
            ],
            compiler_params=pltpu.CompilerParams(
                collective_id=0, has_side_effects=True, vmem_limit_bytes=60000 * 1024
            ),
        )(
            owner_row, selected, dest_slot, candidates, patch_weight.T, positions.T,
            attn_gain, mlp_gain, qkv, out_weight, up_weight, down_weight,
        )

    return jax.shard_map(
        local,
        mesh=mesh,
        in_specs=(
            P("dp", "mp", None), P(), P(), P(), P(None, "mp"), P(None, "mp"), P(None, None, "mp"),
            P("mp", None), P(), P(), P(None, "mp"), P("mp", None),
        ),
        out_specs=P("dp", "mp", None),
        check_vma=False,
    )
```
